32 devices in a mesh: ep: 8 (over z, y), dp: 4 (over x, core).
Axes of the slice: x: 2, y: 2, z: 4, core: 2. Of those that a mesh axis runs over, the one named last changes fastest.
Arguments:
- tokens: bfloat16 [6144, 2880], P(('ep', 'dp')), may hold values from -64 to 64
- out_grad: bfloat16 [6144, 2880], P(('ep', 'dp')), may hold values from -6 to 6
- indices: int32 [6144, 4], P(('ep', 'dp')), may hold values from 0 to 31, as said below
- expert_rows: bfloat16 [4, 32, 8, 36, 2880], P('dp', 'ep'), may hold values from -0.111328125 to 0.111328125
- router_weight: bfloat16 [2880, 32], replicated, may hold values from -1 to 1
- router_bias: float32 [32], replicated, may hold values from -3 to 3
- balance_scale: float32 [1], replicated, may hold values from 64 to 256
Outputs:
- token_grad: bfloat16 [6144, 2880], P(('ep', 'dp'))
- weight_grad: float32 [2880, 32], P('dp', 'ep')
- balance_loss: float32 [1], replicated
The draws below stay inside these ranges and needn't reach their ends.
Inputs may be any that keep to these rules, and one draw needn't show every extreme that they name: `indices`: each row names 4 different experts. Within the 192 rows of one device no expert is named by more than 36 rows, and some expert is named by exactly 36 rows. Within the rows of one device the 4 experts of one ep index (experts j * 4 to j * 4 + 3) are named by at most 108 rows together, and those of some ep index by exactly 108. Every expert is named by some row of every device.
All inputs are finite; a program needn't handle non-finite values.
Results may differ from the reference program's by a relative error of at most 0.0014.
The reference program's roundings to bfloat16 on the way (of `picked` and `logit_grad`) count: a program that leaves them out, or rounds other values in their place, can miss the bound.
Values may be sent and summed in bfloat16 or wider, within the bound.
A program may use at most 128 MiB of HBM per device.

```python
import math
import jax
import jax.numpy as jnp
from jax import lax

D = 2880
K = 4
EXP_DEV = 4
TOK_DEV = 192
E = 32
CAP = 36
TOKENS = 6144
N_EP = 8
N_DP = 4


def router_table(key):
    sub_key = jax.random.fold_in(key, 11)
    scale = D ** (-0.5)
    return jnp.clip(jax.random.normal(sub_key, (D, E), jnp.float32) * scale, -6.0 * scale, 6.0 * scale)


def draw_router_weight(key, part):
    return router_table(key).astype(jnp.bfloat16)


def block_offsets(key, table_rows):
    pick_key = jax.random.fold_in(key, 29)
    picks = jax.random.randint(pick_key, (N_EP * N_DP, 8), 0, E)
    columns = jnp.take(table_rows.T, picks.reshape(-1), axis=0).reshape(N_EP * N_DP, 8, D)
    per_block = 4.0 * jnp.sum(columns, axis=1)
    return jnp.repeat(per_block, TOK_DEV, axis=0)


def draw_tokens(key, part):
    sub_key = jax.random.fold_in(key, 23)
    table_rows = router_table(key)
    shifted = block_offsets(key, table_rows)
    result = jnp.clip(jax.random.normal(sub_key, (TOKENS, D), jnp.float32), -6.0, 6.0) + shifted
    return jnp.clip(result, -64.0, 64.0).astype(jnp.bfloat16)


def route_block(block_key, common_key):
    key_shift, key_rows, key_cols = jax.random.split(block_key, 3)
    key_heavy, key_inner = jax.random.split(common_key, 2)
    third = CAP // 3
    group_order = jax.random.permutation(key_heavy, N_EP)
    heavy = (group_order % 2 == 0)[:, None]
    shift = jax.random.randint(key_shift, (N_EP, 1), 0, third + 1)
    heavy_loads = jnp.concatenate([jnp.full((N_EP, 2), CAP, jnp.int32), 2 * third - shift, third + shift], axis=1)
    light_loads = jnp.concatenate([jnp.full((N_EP, 1), CAP, jnp.int32), 2 * third - shift, third + shift, jnp.full((N_EP, 1), third, jnp.int32)], axis=1)
    pattern = jnp.where(heavy, heavy_loads, light_loads).astype(jnp.int32)
    inner_scores = jax.random.randint(key_inner, (N_EP, EXP_DEV), 0, 1 << 20) * EXP_DEV + jnp.arange(EXP_DEV, dtype=jnp.int32)[None, :]
    inner_order = jnp.argsort(inner_scores, axis=1)
    loads = jnp.take_along_axis(pattern, inner_order, axis=1).reshape(E)
    bounds = jnp.cumsum(loads)
    positions = jnp.arange(TOK_DEV * K, dtype=jnp.int32)
    labels = jnp.searchsorted(bounds, positions, side='right').astype(jnp.int32)
    grid = labels.reshape(K, TOK_DEV).T
    row_order = jax.random.permutation(key_rows, TOK_DEV)
    grid = jnp.take(grid, row_order, axis=0)
    col_scores = jax.random.randint(key_cols, (TOK_DEV, K), 0, 1 << 20) * K + jnp.arange(K, dtype=jnp.int32)[None, :]
    col_order = jnp.argsort(col_scores, axis=1)
    return jnp.take_along_axis(grid, col_order, axis=1).astype(jnp.int32)


def draw_indices(key, part):
    base_key = jax.random.fold_in(key, 37)
    common_key = jax.random.fold_in(key, 41)
    block_ids = jnp.arange(N_EP * N_DP, dtype=jnp.int32)
    blocks = jax.vmap(lambda block_id: route_block(jax.random.fold_in(base_key, block_id), common_key))(block_ids)
    return blocks.reshape(TOKENS, K).astype(jnp.int32)


def block_levels(key, extent, shards, least, largest):
    factor_of, own = 1.0, jax.random.fold_in(key, 6)
    for position, parts in shards:
        draws = jnp.exp(jax.random.uniform(jax.random.fold_in(own, position), (parts,), jnp.float32, least / len(shards), largest / len(shards)))
        factor_of = factor_of * jnp.repeat(draws, extent[position] // parts).reshape([-1 if axis == position else 1 for axis in range(len(extent))])
    return factor_of


def gaussian(stream_key, extent, scale, bound, pieces=(), kind=jnp.bfloat16):
    entries = jax.random.normal(stream_key, extent, jnp.float32) * scale
    if len(pieces) > 0:
        entries = block_levels(stream_key, extent, pieces, -0.22, 0.18) * entries
    return jnp.clip(entries, min=-bound, max=bound).astype(kind)


def setup_inputs(seed: int = 0) -> dict:
    splits = jax.random.split(jax.random.key(seed), 8)
    return {
        "tokens": draw_tokens(jax.random.fold_in(splits[7], 71), 0),
        "out_grad": gaussian(splits[1], (TOKENS, D), 1.0, 6.0, ((0, 32),)),
        "indices": draw_indices(jax.random.fold_in(splits[7], 71), 0),
        "expert_rows": gaussian(splits[3], (N_DP, E, N_EP, CAP, D), (D ** -0.5), 0.111328125, ((0, 4), (1, 8))),
        "router_weight": draw_router_weight(jax.random.fold_in(splits[7], 71), 0),
        "router_bias": gaussian(splits[5], (E,), 0.5, 3.0, (), jnp.float32),
        "balance_scale": jnp.clip(jnp.exp(jax.random.uniform(splits[6], (1,), jnp.float32, math.log(64.0), math.log(256.0))), 64.0, 256.0),
    }


def reference(tokens, out_grad, indices, expert_rows, router_weight, router_bias, balance_scale):
    logits = jnp.dot(tokens, router_weight, preferred_element_type=jnp.float32) + router_bias
    probability = jax.nn.softmax(logits, axis=-1)
    expert_ids = jnp.arange(E, dtype=jnp.int32)
    onehot = (indices[:, :, None] == expert_ids[None, None, :]).astype(jnp.float32)
    counts = lax.optimization_barrier(jnp.sum(onehot, axis=(0, 1)))
    prob_mean = lax.optimization_barrier(jnp.sum(probability, axis=0)) / TOKENS
    share_of = counts / (TOKENS * K)
    balance_loss = (E * jnp.sum(share_of * prob_mean)).reshape(1)

    def block_dots(block_id):
        ep_index = block_id // N_DP
        dp_index = block_id % N_DP
        cotangent = lax.dynamic_slice_in_dim(out_grad, block_id * TOK_DEV, TOK_DEV, 0)
        chosen_ids = lax.dynamic_slice_in_dim(indices, block_id * TOK_DEV, TOK_DEV, 0)
        group_rows = lax.dynamic_index_in_dim(expert_rows, dp_index, 0, keepdims=False)
        table_rows = lax.dynamic_index_in_dim(group_rows, ep_index, 1, keepdims=False)
        named_by = lax.optimization_barrier(jnp.sum((chosen_ids[:, :, None] == expert_ids[None, None, :]).astype(jnp.int32), axis=1))
        before = jnp.cumsum(named_by, axis=0) - named_by
        slot_index = jnp.take_along_axis(before, chosen_ids, axis=1)
        row_index = (chosen_ids * CAP + slot_index).astype(jnp.int32)
        picked = table_rows.reshape(E * CAP, D)[row_index]
        return jnp.einsum('td,tkd->tk', cotangent.astype(jnp.float32), picked.astype(jnp.float32))
    pair_dots = lax.map(block_dots, jnp.arange(N_EP * N_DP, dtype=jnp.int32)).reshape(TOKENS, K)
    chosen_logits = jnp.take_along_axis(logits, indices, axis=1)
    mix_weight = jax.nn.softmax(chosen_logits, axis=-1)
    sel_grad = mix_weight * (pair_dots - lax.optimization_barrier(jnp.sum(mix_weight * pair_dots, axis=1, keepdims=True)))
    balance_push = balance_scale[0] * E * share_of
    spread = probability * (balance_push[None, :] - lax.optimization_barrier(jnp.sum(probability * balance_push[None, :], axis=1, keepdims=True)))
    logit_grad = (spread + lax.optimization_barrier(jnp.sum(onehot * sel_grad[:, :, None], axis=1))).astype(jnp.bfloat16)
    token_grad = jnp.dot(logit_grad, router_weight.T, preferred_element_type=jnp.float32).astype(jnp.bfloat16)
    weight_grad = jnp.dot(tokens.T, logit_grad, preferred_element_type=jnp.float32) / math.sqrt(TOKENS)
    return (token_grad, weight_grad, balance_loss)
```

```python
import functools
import math

import jax
import jax.numpy as jnp
from jax import lax
from jax.experimental import pallas as pl
from jax.experimental.pallas import tpu as pltpu
from jax.sharding import PartitionSpec as P

MESH = pl.DeviceIdType.MESH
F32 = jnp.float32
BF16 = jnp.bfloat16
CHUNK = 768


def dot_nt(x, y, precision=None):
    return lax.dot_general(
        x, y, (((1,), (1,)), ((), ())), preferred_element_type=F32, precision=precision
    )


def dot_nn(x, y, precision=None):
    return lax.dot_general(
        x, y, (((1,), (0,)), ((), ())), preferred_element_type=F32, precision=precision
    )


def kernel(cfg, *refs):
    ep, dp, tok_dev, chosen, experts, exp_dev, cap, packed, widths, token_total = cfg
    line = ep // 2
    chunks = len(widths)
    starts = [sum(widths[:c]) for c in range(chunks)]
    (idx_in, grad_in, rows_in, tok_in, wt_in, bias_in, scale_in, lg_out, wg_out, loss_out) = refs[:10]
    refs = refs[10:]
    xb = refs[:chunks]
    lsend = refs[chunks:2 * chunks]
    lrecv = refs[2 * chunks:3 * chunks]
    (rows_v, idx_all, pin, pout, tgt_x, tgt_p, acc_x, acc_p, rst, rbuf, tks, tkr, logit_v, prob_v,
     named_v, st_dp, st_ep, lgd, ws, wr,
     s_rows, s_own, s_idx, r_idx, s_right, s_left, r_x, s_leaf, r_leaf, s_rep, r_rep,
     s_tk, r_tk, s_sd, r_sd, s_se, r_se, s_lg, r_lg, s_w, r_w) = refs[3 * chunks:]
    me = lax.axis_index("ep")
    md = lax.axis_index("dp")
    pos = me // 2
    side = lax.rem(me, 2)
    mate = pos * 2 + 1 - side

    def ep_id(other):
        return (other, md)

    def remote(src, dst, s, r, dev):
        return pltpu.make_async_remote_copy(
            src_ref=src, dst_ref=dst, send_sem=s, recv_sem=r, device_id=dev, device_id_type=MESH
        )

    def ep_peer(s):
        return lax.rem(me + s, ep)

    def dp_peer(s):
        return lax.rem(md + s, dp)

    own = [
        pltpu.make_async_copy(grad_in.at[:, pl.ds(starts[c], widths[c])], xb[c].at[pos], s_own.at[c])
        for c in range(chunks)
    ]
    for copy in own:
        copy.start()
    rows_copy = pltpu.make_async_copy(rows_in.at[0], rows_v, s_rows)
    rows_copy.start()

    barrier = pltpu.get_barrier_semaphore()

    def greet(s, carry):
        pl.semaphore_signal(barrier, inc=1, device_id=ep_id(ep_peer(s)), device_id_type=MESH)
        return carry

    lax.fori_loop(1, ep, greet, 0)
    for s in range(1, dp):
        pl.semaphore_signal(barrier, inc=1, device_id=(me, dp_peer(s)), device_id_type=MESH)
    pl.semaphore_wait(barrier, ep - 1 + dp - 1)

    def idx_copy(s):
        return remote(idx_in, idx_all.at[me], s_idx.at[s], r_idx.at[me], ep_id(ep_peer(s)))

    def idx_arrival(s):
        src = lax.rem(me + ep - s, ep)
        return remote(idx_in, idx_all.at[src], s_idx.at[s], r_idx.at[src], ep_id(src))

    def loop_ep(fn):
        def body(s, carry):
            fn(s)
            return carry
        lax.fori_loop(1, ep, body, 0)

    def to_right(q, c):
        return remote(xb[c].at[q], xb[c].at[q], s_right.at[q, c], r_x.at[q, c], ep_id(me + 2))

    def to_left(q, c):
        return remote(xb[c].at[q], xb[c].at[q], s_left.at[q, c], r_x.at[q, c], ep_id(me - 2))

    def leaf(q, c):
        return remote(lsend[c].at[q], lrecv[c].at[q], s_leaf.at[q, c], r_leaf.at[q, c], ep_id(mate))

    def reply(j):
        return remote(rst.at[j], rbuf.at[me], s_rep.at[j], r_rep.at[me], ep_id(j))

    loop_ep(lambda s: idx_copy(s).start())
    for c in range(chunks):
        own[c].wait()

        @pl.when(pos < line - 1)
        def _():
            to_right(pos, c).start()

        @pl.when(pos > 0)
        def _():
            to_left(pos, c).start()

    part = tok_in.shape[1] // dp
    for d in range(dp):
        tks[d] = tok_in[:, d * part:(d + 1) * part]

    idx = idx_in[...]
    expert_row = lax.broadcasted_iota(jnp.int32, (experts, tok_dev), 0)
    named = jnp.zeros((experts, tok_dev), F32)
    for k in range(chosen):
        named = named + jnp.where(idx[k:k + 1, :] == expert_row, 1.0, 0.0)
    logits = dot_nt(wt_in[...], tok_in[...]) + bias_in[...]
    top = jnp.max(logits, axis=0, keepdims=True)
    power = jnp.exp(logits - top)
    prob = power / jnp.sum(power, axis=0, keepdims=True)
    logit_v[...] = logits
    prob_v[...] = prob
    named_v[...] = named
    ones = jnp.ones((8, tok_dev), F32)
    count_row = dot_nt(ones, named, lax.Precision.HIGHEST)
    prob_row = dot_nt(ones, prob, lax.Precision.HIGHEST)
    stat_row = lax.broadcasted_iota(jnp.int32, (8, experts), 0)
    st_dp[md] = jnp.where(stat_row == 0, count_row, prob_row)

    def tk_copy(s):
        return remote(tks.at[dp_peer(s)], tkr.at[md], s_tk.at[s], r_tk.at[md], (me, dp_peer(s)))

    def tk_arrival(s):
        src = lax.rem(md + dp - s, dp)
        return remote(tks.at[src], tkr.at[src], s_tk.at[s], r_tk.at[src], (me, src))

    def sd_copy(s):
        return remote(st_dp.at[md], st_dp.at[md], s_sd.at[s], r_sd.at[md], (me, dp_peer(s)))

    def sd_arrival(s):
        src = lax.rem(md + dp - s, dp)
        return remote(st_dp.at[src], st_dp.at[src], s_sd.at[s], r_sd.at[src], (me, src))

    for s in range(1, dp):
        sd_copy(s).start()
    for s in range(1, dp):
        tk_copy(s).start()
    tkr[md] = tks[md]

    t_from = lax.broadcasted_iota(jnp.int32, (tok_dev, tok_dev), 0)
    t_to = lax.broadcasted_iota(jnp.int32, (tok_dev, tok_dev), 1)
    upper = jnp.where(t_from < t_to, 1.0, 0.0).astype(BF16)
    row8 = lax.broadcasted_iota(jnp.int32, (8, tok_dev), 0)
    slot_p = lax.broadcasted_iota(jnp.int32, (packed, tok_dev), 0).astype(F32)

    def plan(table, group):
        who = jnp.where(row8 < exp_dev, group * exp_dev + row8, -2)
        hit = jnp.zeros((8, tok_dev), F32)
        for k in range(chosen):
            hit = hit + jnp.where(table[k:k + 1, :] == who, 1.0, 0.0)
        need = jnp.max(hit, axis=0, keepdims=True)
        stack = jnp.where(row8 == exp_dev, need, hit)
        before = dot_nn(stack.astype(BF16), upper)
        place = jnp.where(need > 0.5, before[exp_dev:exp_dev + 1, :], -1.0)
        target = jnp.where(hit > 0.5, before, -1.0)
        pack = jnp.where(slot_p == place, 1.0, 0.0).astype(BF16)
        return target, pack

    idx_all[me] = idx
    loop_ep(lambda s: idx_arrival(s).wait_recv())

    def plans(q, carry):
        table = idx_all[q * 2 + side]
        target, _ = plan(table, me)
        tgt_x[q] = target
        _, pack = plan(table, mate)
        pout[q] = pack
        target, pack = plan(idx_all[q * 2 + 1 - side], me)
        pin[q] = pack
        tgt_p[q] = dot_nt((target + 1.0).astype(BF16), pack) - 1.0
        acc_x[q] = jnp.zeros((8, tok_dev), F32)
        acc_p[q] = jnp.zeros((8, packed), F32)
        return carry

    lax.fori_loop(0, line, plans, 0)
    rows_copy.wait()

    def gathered(j, c, block, target, count):
        slot = lax.broadcasted_iota(jnp.int32, (cap, count), 0).astype(F32)
        row = lax.broadcasted_iota(jnp.int32, (8, count), 0)
        out = jnp.zeros((8, count), F32)
        for e in range(exp_dev):
            table = rows_v[e, j, :, starts[c]:starts[c] + widths[c]]
            dots = dot_nt(table, block)
            one = jnp.sum(jnp.where(slot == target[e:e + 1, :], dots, 0.0), axis=0, keepdims=True)
            out = jnp.where(row == e, one, out)
        return out

    def give_leaf(q, c):
        lsend[c][q] = dot_nn(pout[q], xb[c][q]).astype(BF16)
        leaf(q, c).start()

    def use_block(q, c):
        acc_x[q] += gathered(q * 2 + side, c, xb[c][q], tgt_x[q], tok_dev)

    def use_leaf(q, c):
        leaf(q, c).wait_recv()
        acc_p[q] += gathered(q * 2 + 1 - side, c, lrecv[c][q], tgt_p[q], packed)

    def answer(j, value):
        rst[j] = value
        reply(j).start()

    def done_block(q):
        answer(q * 2 + side, acc_x[q])

    def done_leaf(q):
        answer(q * 2 + 1 - side, dot_nn(acc_p[q], pin[q].astype(F32), lax.Precision.HIGHEST))

    def leaf_step(s, c):
        def go(q):
            use_leaf(q, c)
            if c == chunks - 1:
                done_leaf(q)
        if s == 0:
            go(pos)
            return

        @pl.when(pos - s >= 0)
        def _():
            go(pos - s)

        @pl.when(pos + s < line)
        def _():
            go(pos + s)

    lag = 2
    steps = [(s, c) for s in range(line) for c in range(chunks)]
    for n, (s, c) in enumerate(steps):
        if s == 0:
            give_leaf(pos, c)
            use_block(pos, c)
            if c == chunks - 1:
                rbuf[me] = acc_x[pos]
        else:
            @pl.when(pos - s >= 0)
            def _():
                q = pos - s
                to_right(q, c).wait_recv()

                @pl.when(pos < line - 1)
                def _():
                    to_right(q, c).start()

            @pl.when(pos + s < line)
            def _():
                q = pos + s
                to_left(q, c).wait_recv()

                @pl.when(pos > 0)
                def _():
                    to_left(q, c).start()

            for q, ok in ((pos - s, pos - s >= 0), (pos + s, pos + s < line)):
                @pl.when(ok)
                def _(q=q):
                    give_leaf(q, c)

            for q, ok in ((pos - s, pos - s >= 0), (pos + s, pos + s < line)):
                @pl.when(ok)
                def _(q=q):
                    use_block(q, c)
                    if c == chunks - 1:
                        done_block(q)
        if n >= lag:
            leaf_step(*steps[n - lag])
        if n == 1:
            for s_ in range(1, dp):
                sd_arrival(s_).wait_recv()
            total = st_dp[0]
            for d in range(1, dp):
                total = total + st_dp[d]
            st_ep[me] = total
            loop_ep(lambda s_: remote(st_ep.at[me], st_ep.at[me], s_se.at[s_], r_se.at[me], ep_id(ep_peer(s_))).start())
    for n in range(len(steps) - lag, len(steps)):
        leaf_step(*steps[n])

    def se_arrival(s_):
        src = lax.rem(me + ep - s_, ep)
        remote(st_ep.at[src], st_ep.at[src], s_se.at[s_], r_se.at[src], ep_id(src)).wait_recv()

    loop_ep(se_arrival)
    stats = lax.fori_loop(1, ep, lambda j, acc: acc + st_ep[j], st_ep[0])
    share = stats[0:1, :] / (token_total * chosen)
    mean = stats[1:2, :] / token_total
    loss_out[...] = experts * jnp.sum(share * mean, axis=1, keepdims=True)
    push_row = scale_in[0] * experts * share
    eye_r = lax.broadcasted_iota(jnp.int32, (experts, experts), 0)
    eye_c = lax.broadcasted_iota(jnp.int32, (experts, experts), 1)
    push = jnp.sum(jnp.where(eye_r == eye_c, push_row, 0.0), axis=1, keepdims=True)
    prob = prob_v[...]
    spread = prob * (push - jnp.sum(prob * push, axis=0, keepdims=True))
    named = named_v[...]
    logits = logit_v[...]
    high = jnp.max(jnp.where(named > 0.5, logits, -jnp.inf), axis=0, keepdims=True)
    mix = jnp.where(named > 0.5, jnp.exp(jnp.minimum(logits - high, 0.0)), 0.0)
    mix = mix / jnp.sum(mix, axis=0, keepdims=True)

    def rep_arrival(s_):
        src = lax.rem(me + ep - s_, ep)
        remote(rst.at[src], rbuf.at[src], s_rep.at[src], r_rep.at[src], ep_id(src)).wait_recv()

    loop_ep(rep_arrival)
    dots = jnp.concatenate([rbuf[j, 0:exp_dev, :] for j in range(ep)], axis=0)
    sel = mix * (dots - jnp.sum(mix * dots, axis=0, keepdims=True))
    grad = (spread + sel).astype(BF16)
    lg_out[...] = grad
    lgd[md] = grad

    def lg_copy(s):
        return remote(lgd.at[md], lgd.at[md], s_lg.at[s], r_lg.at[md], (me, dp_peer(s)))

    def lg_arrival(s):
        src = lax.rem(md + dp - s, dp)
        return remote(lgd.at[src], lgd.at[src], s_lg.at[s], r_lg.at[src], (me, src))

    for s in range(1, dp):
        lg_copy(s).start()
    for s in range(1, dp):
        tk_arrival(s).wait_recv()
    for s in range(1, dp):
        lg_arrival(s).wait_recv()
    term = dot_nn(lgd[0], tkr[0])
    for d in range(1, dp):
        term = term + dot_nn(lgd[d], tkr[d])
    for j in range(ep):
        ws[j] = term[j * exp_dev:(j + 1) * exp_dev, :]
    wr[me] = ws[me]
    loop_ep(lambda s_: remote(ws.at[ep_peer(s_)], wr.at[me], s_w.at[s_], r_w.at[me], ep_id(ep_peer(s_))).start())

    def w_arrival(s_):
        src = lax.rem(me + ep - s_, ep)
        remote(ws.at[src], wr.at[src], s_w.at[s_], r_w.at[src], ep_id(src)).wait_recv()

    loop_ep(w_arrival)
    out = lax.fori_loop(1, ep, lambda j, acc: acc + wr[j], wr[0])
    wg_out[...] = out / math.sqrt(token_total)

    loop_ep(lambda s_: idx_copy(s_).wait_send())
    loop_ep(lambda s_: remote(st_ep.at[me], st_ep.at[me], s_se.at[s_], r_se.at[me], ep_id(ep_peer(s_))).wait_send())
    loop_ep(lambda s_: reply(ep_peer(s_)).wait_send())
    loop_ep(lambda s_: remote(ws.at[ep_peer(s_)], wr.at[me], s_w.at[s_], r_w.at[me], ep_id(ep_peer(s_))).wait_send())
    for s in range(1, dp):
        sd_copy(s).wait_send()
        tk_copy(s).wait_send()
        lg_copy(s).wait_send()

    def drain(q, carry):
        for c in range(chunks):
            leaf(q, c).wait_send()

            @pl.when(jnp.logical_and(q <= pos, pos < line - 1))
            def _():
                to_right(q, c).wait_send()

            @pl.when(jnp.logical_and(q >= pos, pos > 0))
            def _():
                to_left(q, c).wait_send()
        return carry

    lax.fori_loop(0, line, drain, 0)


def on_device(tokens, out_grad, indices, expert_rows, router_weight, router_bias, balance_scale):
    tok_dev, width = tokens.shape
    chosen = indices.shape[1]
    experts = router_weight.shape[1]
    exp_dev, cap = expert_rows.shape[1], expert_rows.shape[3]
    ep = lax.axis_size("ep")
    dp = lax.axis_size("dp")
    line = ep // 2
    packed = -(-min(tok_dev, (exp_dev - 1) * cap) // 16) * 16
    widths = tuple(min(CHUNK, width - s) for s in range(0, width, CHUNK))
    chunks = len(widths)
    cfg = (ep, dp, tok_dev, chosen, experts, exp_dev, cap, packed, widths, tok_dev * ep * dp)
    part = width // dp
    idx_t = jnp.pad(indices.T, ((0, 8 - chosen), (0, 0)), constant_values=-1)
    vmem = pl.BlockSpec(memory_space=pltpu.VMEM)
    hbm = pl.BlockSpec(memory_space=pl.ANY)
    smem = pl.BlockSpec(memory_space=pltpu.SMEM)
    dma = pltpu.SemaphoreType.DMA
    scratch = [pltpu.VMEM((line, tok_dev, w), BF16) for w in widths]
    scratch += [pltpu.VMEM((line, packed, w), BF16) for w in widths]
    scratch += [pltpu.VMEM((line, packed, w), BF16) for w in widths]
    scratch += [
        pltpu.VMEM(expert_rows.shape[1:], BF16),
        pltpu.VMEM((ep, 8, tok_dev), jnp.int32),
        pltpu.VMEM((line, packed, tok_dev), BF16),
        pltpu.VMEM((line, packed, tok_dev), BF16),
        pltpu.VMEM((line, 8, tok_dev), F32),
        pltpu.VMEM((line, 8, packed), F32),
        pltpu.VMEM((line, 8, tok_dev), F32),
        pltpu.VMEM((line, 8, packed), F32),
        pltpu.VMEM((ep, 8, tok_dev), F32),
        pltpu.VMEM((ep, 8, tok_dev), F32),
        pltpu.VMEM((dp, tok_dev, part), BF16),
        pltpu.VMEM((dp, tok_dev, part), BF16),
        pltpu.VMEM((experts, tok_dev), F32),
        pltpu.VMEM((experts, tok_dev), F32),
        pltpu.VMEM((experts, tok_dev), F32),
        pltpu.VMEM((dp, 8, experts), F32),
        pltpu.VMEM((ep, 8, experts), F32),
        pltpu.VMEM((dp, experts, tok_dev), BF16),
        pltpu.VMEM((ep, exp_dev, part), F32),
        pltpu.VMEM((ep, exp_dev, part), F32),
        dma, dma((chunks,)), dma((ep,)), dma((ep,)),
        dma((line, chunks)), dma((line, chunks)), dma((line, chunks)),
        dma((line, chunks)), dma((line, chunks)), dma((ep,)), dma((ep,)),
        dma((dp,)), dma((dp,)), dma((dp,)), dma((dp,)), dma((ep,)), dma((ep,)),
        dma((dp,)), dma((dp,)), dma((ep,)), dma((ep,)),
    ]
    lg, wg, loss = pl.pallas_call(
        functools.partial(kernel, cfg),
        name="router_backward",
        out_shape=(
            jax.ShapeDtypeStruct((experts, tok_dev), BF16),
            jax.ShapeDtypeStruct((exp_dev, part), F32),
            jax.ShapeDtypeStruct((1, 1), F32),
        ),
        in_specs=[vmem, hbm, hbm, vmem, vmem, vmem, smem],
        out_specs=(vmem, vmem, vmem),
        scratch_shapes=scratch,
        compiler_params=pltpu.CompilerParams(
            collective_id=0, has_side_effects=True, vmem_limit_bytes=56 * 1024 * 1024
        ),
    )(idx_t, out_grad, expert_rows, tokens, router_weight.T, router_bias.reshape(experts, 1), balance_scale)
    token_grad = lax.dot_general(
        lg, router_weight, (((0,), (1,)), ((), ())), preferred_element_type=F32
    ).astype(BF16)
    return (token_grad, wg.T, loss.reshape(1))


def solution(mesh):
    placed = (
        P(("ep", "dp"), None),
        P(("ep", "dp"), None),
        P(("ep", "dp"), None),
        P("dp", "ep", None, None, None),
        P(),
        P(),
        P(),
    )
    return jax.shard_map(
        on_device,
        mesh=mesh,
        in_specs=placed,
        out_specs=(P(("ep", "dp"), None), P("dp", "ep"), P()),
        check_vma=False,
    )
```

```python
import functools
import math

import jax
import jax.numpy as jnp
from jax import lax
from jax.experimental import pallas as pl
from jax.experimental.pallas import tpu as pltpu
from jax.sharding import PartitionSpec as P

MESH = pl.DeviceIdType.MESH
F32 = jnp.float32
BF16 = jnp.bfloat16
CHUNK = 768


def dot_nt(x, y, precision=None):
    return lax.dot_general(
        x, y, (((1,), (1,)), ((), ())), preferred_element_type=F32, precision=precision
    )


def dot_nn(x, y, precision=None):
    return lax.dot_general(
        x, y, (((1,), (0,)), ((), ())), preferred_element_type=F32, precision=precision
    )


def kernel(cfg, *refs):
    ep, dp, tok_dev, chosen, experts, exp_dev, cap, packed, widths, token_total = cfg
    line = ep // 2
    chunks = len(widths)
    starts = [sum(widths[:c]) for c in range(chunks)]
    (idx_in, grad_in, rows_in, tok_in, wt_in, bias_in, scale_in, lg_out, wg_out, loss_out) = refs[:10]
    refs = refs[10:]
    xb = refs[:chunks]
    lsend = refs[chunks:2 * chunks]
    lrecv = refs[2 * chunks:3 * chunks]
    rows_v = refs[3 * chunks:4 * chunks]
    (rows_raw, piled, idx_all, pin, pout, tgt_x, tgt_p, acc_x, acc_p, rst, rbuf, tks, tkr, logit_v, prob_v,
     named_v, st_dp, st_ep, lgd, ws, wr,
     s_rows, s_own, s_idx, r_idx, s_right, s_left, r_x, s_leaf, r_leaf, s_rep, r_rep,
     s_tk, r_tk, s_sd, r_sd, s_se, r_se, s_lg, r_lg, s_w, r_w) = refs[4 * chunks:]
    me = lax.axis_index("ep")
    md = lax.axis_index("dp")
    pos = me // 2
    side = lax.rem(me, 2)
    mate = pos * 2 + 1 - side

    def ep_id(other):
        return (other, md)

    def remote(src, dst, s, r, dev):
        return pltpu.make_async_remote_copy(
            src_ref=src, dst_ref=dst, send_sem=s, recv_sem=r, device_id=dev, device_id_type=MESH
        )

    def ep_peer(s):
        return lax.rem(me + s, ep)

    def dp_peer(s):
        return lax.rem(md + s, dp)

    own = [
        pltpu.make_async_copy(grad_in.at[:, pl.ds(starts[c], widths[c])], xb[c].at[pos], s_own.at[c])
        for c in range(chunks)
    ]
    for copy in own:
        copy.start()
    rows_copy = pltpu.make_async_copy(rows_in, rows_raw, s_rows)
    rows_copy.start()

    barrier = pltpu.get_barrier_semaphore()

    def greet(s, carry):
        pl.semaphore_signal(barrier, inc=1, device_id=ep_id(ep_peer(s)), device_id_type=MESH)
        return carry

    lax.fori_loop(1, ep, greet, 0)
    for s in range(1, dp):
        pl.semaphore_signal(barrier, inc=1, device_id=(me, dp_peer(s)), device_id_type=MESH)
    pl.semaphore_wait(barrier, ep - 1 + dp - 1)

    def idx_copy(s):
        return remote(idx_in, idx_all.at[me], s_idx.at[s], r_idx.at[me], ep_id(ep_peer(s)))

    def idx_arrival(s):
        src = lax.rem(me + ep - s, ep)
        return remote(idx_in, idx_all.at[src], s_idx.at[s], r_idx.at[src], ep_id(src))

    def loop_ep(fn):
        def body(s, carry):
            fn(s)
            return carry
        lax.fori_loop(1, ep, body, 0)

    def to_right(q, c):
        return remote(xb[c].at[q], xb[c].at[q], s_right.at[q, c], r_x.at[q, c], ep_id(me + 2))

    def to_left(q, c):
        return remote(xb[c].at[q], xb[c].at[q], s_left.at[q, c], r_x.at[q, c], ep_id(me - 2))

    def leaf(q, c):
        return remote(lsend[c].at[q], lrecv[c].at[q], s_leaf.at[q, c], r_leaf.at[q, c], ep_id(mate))

    def reply(j):
        return remote(rst.at[j], rbuf.at[me], s_rep.at[j], r_rep.at[me], ep_id(j))

    loop_ep(lambda s: idx_copy(s).start())
    for c in range(chunks):
        own[c].wait()

        @pl.when(pos < line - 1)
        def _():
            to_right(pos, c).start()

        @pl.when(pos > 0)
        def _():
            to_left(pos, c).start()

    part = tok_in.shape[1] // dp
    for d in range(dp):
        tks[d] = tok_in[:, d * part:(d + 1) * part]

    idx = idx_in[...]
    expert_row = lax.broadcasted_iota(jnp.int32, (experts, tok_dev), 0)
    named = jnp.zeros((experts, tok_dev), F32)
    for k in range(chosen):
        named = named + jnp.where(idx[k:k + 1, :] == expert_row, 1.0, 0.0)
    eye_r = lax.broadcasted_iota(jnp.int32, (experts, experts), 0)
    eye_c = lax.broadcasted_iota(jnp.int32, (experts, experts), 1)

    def upright(line_of):
        return jnp.sum(jnp.where(eye_r == eye_c, line_of, 0.0), axis=1, keepdims=True)

    logits = dot_nt(wt_in[...], tok_in[...]) + upright(bias_in[...])
    top = jnp.max(logits, axis=0, keepdims=True)
    power = jnp.exp(logits - top)
    prob = power / jnp.sum(power, axis=0, keepdims=True)
    logit_v[...] = logits
    prob_v[...] = prob
    named_v[...] = named
    ones = jnp.ones((8, tok_dev), F32)
    count_row = dot_nt(ones, named, lax.Precision.HIGHEST)
    prob_row = dot_nt(ones, prob, lax.Precision.HIGHEST)
    stat_row = lax.broadcasted_iota(jnp.int32, (8, experts), 0)
    st_dp[md] = jnp.where(stat_row == 0, count_row, prob_row)

    def tk_copy(s):
        return remote(tks.at[dp_peer(s)], tkr.at[md], s_tk.at[s], r_tk.at[md], (me, dp_peer(s)))

    def tk_arrival(s):
        src = lax.rem(md + dp - s, dp)
        return remote(tks.at[src], tkr.at[src], s_tk.at[s], r_tk.at[src], (me, src))

    def sd_copy(s):
        return remote(st_dp.at[md], st_dp.at[md], s_sd.at[s], r_sd.at[md], (me, dp_peer(s)))

    def sd_arrival(s):
        src = lax.rem(md + dp - s, dp)
        return remote(st_dp.at[src], st_dp.at[src], s_sd.at[s], r_sd.at[src], (me, src))

    for s in range(1, dp):
        sd_copy(s).start()
    for s in range(1, dp):
        tk_copy(s).start()
    tkr[md] = tks[md]

    t_from = lax.broadcasted_iota(jnp.int32, (tok_dev, tok_dev), 0)
    t_to = lax.broadcasted_iota(jnp.int32, (tok_dev, tok_dev), 1)
    upper = jnp.where(t_from < t_to, 1.0, 0.0).astype(BF16)
    row8 = lax.broadcasted_iota(jnp.int32, (8, tok_dev), 0)
    slot_p = lax.broadcasted_iota(jnp.int32, (packed, tok_dev), 0).astype(F32)

    def plan(table, group):
        who = jnp.where(row8 < exp_dev, group * exp_dev + row8, -2)
        hit = jnp.zeros((8, tok_dev), F32)
        for k in range(chosen):
            hit = hit + jnp.where(table[k:k + 1, :] == who, 1.0, 0.0)
        need = jnp.max(hit, axis=0, keepdims=True)
        stack = jnp.where(row8 == exp_dev, need, hit)
        before = dot_nn(stack.astype(BF16), upper)
        place = jnp.where(need > 0.5, before[exp_dev:exp_dev + 1, :], -1.0)
        target = jnp.where(hit > 0.5, before, -1.0)
        pack = jnp.where(slot_p == place, 1.0, 0.0).astype(BF16)
        return target, pack

    idx_all[me] = idx
    loop_ep(lambda s: idx_arrival(s).wait_recv())

    def plans(q, carry):
        table = idx_all[q * 2 + side]
        target, _ = plan(table, me)
        tgt_x[q] = target
        _, pack = plan(table, mate)
        pout[q] = pack
        target, pack = plan(idx_all[q * 2 + 1 - side], me)
        pin[q] = pack
        tgt_p[q] = dot_nt((target + 1.0).astype(BF16), pack) - 1.0
        acc_x[q] = jnp.zeros((8, tok_dev), F32)
        acc_p[q] = jnp.zeros((8, packed), F32)
        return carry

    lax.fori_loop(0, line, plans, 0)
    rows_copy.wait()

    deep = piled.shape[1] // ep
    slot_r = lax.broadcasted_iota(jnp.int32, (deep, cap * ep), 0)
    lies = lax.broadcasted_iota(jnp.int32, (deep, cap * ep), 1)
    order = jnp.concatenate(
        [jnp.where(jnp.logical_and(lies == slot_r * ep + j, slot_r < cap), 1.0, 0.0) for j in range(ep)], axis=0
    ).astype(BF16)
    spare = rows_v[0].shape[1] - exp_dev * cap

    def sort_rows(c):
        w = widths[c]
        for e in range(exp_dev):
            piled[e, :, 0:w] = dot_nn(order, rows_raw[e, :, starts[c]:starts[c] + w])

        def put(j, carry):
            at = pl.ds(pl.multiple_of(j * deep, 8), deep)
            pieces = [piled[e, at, 0:w][0:cap, :] for e in range(exp_dev)]
            if spare:
                pieces.append(jnp.zeros((spare, w), F32))
            rows_v[c][j] = jnp.concatenate(pieces, axis=0).astype(BF16)
            return carry

        lax.fori_loop(0, ep, put, 0)

    def gathered(table, block, target, count):
        height = table.shape[0]
        slot = lax.broadcasted_iota(jnp.int32, (height, count), 0).astype(F32)
        row = lax.broadcasted_iota(jnp.int32, (8, count), 0)
        dots = dot_nt(table, block)
        out = jnp.zeros((8, count), F32)
        for e in range(exp_dev):
            want = jnp.where(target[e:e + 1, :] >= 0.0, target[e:e + 1, :] + e * cap, -1.0)
            one = jnp.sum(jnp.where(slot == want, dots, 0.0), axis=0, keepdims=True)
            out = jnp.where(row == e, one, out)
        return out

    def give_leaf(q, c):
        lsend[c][q] = dot_nn(pout[q], xb[c][q]).astype(BF16)
        leaf(q, c).start()

    def use_block(q, c):
        acc_x[q] += gathered(rows_v[c][q * 2 + side], xb[c][q], tgt_x[q], tok_dev)

    def use_leaf(q, c):
        leaf(q, c).wait_recv()
        acc_p[q] += gathered(rows_v[c][q * 2 + 1 - side], lrecv[c][q], tgt_p[q], packed)

    def answer(j, value):
        rst[j] = value
        reply(j).start()

    def done_block(q):
        answer(q * 2 + side, acc_x[q])

    def done_leaf(q):
        answer(q * 2 + 1 - side, dot_nn(acc_p[q], pin[q].astype(F32), lax.Precision.HIGHEST))

    def leaf_step(s, c):
        def go(q):
            use_leaf(q, c)
            if c == chunks - 1:
                done_leaf(q)
        if s == 0:
            go(pos)
            return

        @pl.when(pos - s >= 0)
        def _():
            go(pos - s)

        @pl.when(pos + s < line)
        def _():
            go(pos + s)

    lag = 2
    steps = [(s, c) for s in range(line) for c in range(chunks)]
    for n, (s, c) in enumerate(steps):
        if s == 0:
            give_leaf(pos, c)
            sort_rows(c)
            use_block(pos, c)
            if c == chunks - 1:
                rbuf[me] = acc_x[pos]
        else:
            @pl.when(pos - s >= 0)
            def _():
                q = pos - s
                to_right(q, c).wait_recv()

                @pl.when(pos < line - 1)
                def _():
                    to_right(q, c).start()

            @pl.when(pos + s < line)
            def _():
                q = pos + s
                to_left(q, c).wait_recv()

                @pl.when(pos > 0)
                def _():
                    to_left(q, c).start()

            for q, ok in ((pos - s, pos - s >= 0), (pos + s, pos + s < line)):
                @pl.when(ok)
                def _(q=q):
                    give_leaf(q, c)

            for q, ok in ((pos - s, pos - s >= 0), (pos + s, pos + s < line)):
                @pl.when(ok)
                def _(q=q):
                    use_block(q, c)
                    if c == chunks - 1:
                        done_block(q)
        if n >= lag:
            leaf_step(*steps[n - lag])
        if n == 1:
            for s_ in range(1, dp):
                sd_arrival(s_).wait_recv()
            total = st_dp[0]
            for d in range(1, dp):
                total = total + st_dp[d]
            st_ep[me] = total
            loop_ep(lambda s_: remote(st_ep.at[me], st_ep.at[me], s_se.at[s_], r_se.at[me], ep_id(ep_peer(s_))).start())
    for n in range(len(steps) - lag, len(steps)):
        leaf_step(*steps[n])

    def se_arrival(s_):
        src = lax.rem(me + ep - s_, ep)
        remote(st_ep.at[src], st_ep.at[src], s_se.at[s_], r_se.at[src], ep_id(src)).wait_recv()

    loop_ep(se_arrival)
    stats = lax.fori_loop(1, ep, lambda j, acc: acc + st_ep[j], st_ep[0])
    share = stats[0:1, :] / (token_total * chosen)
    mean = stats[1:2, :] / token_total
    loss_out[...] = experts * jnp.sum(share * mean, axis=1, keepdims=True)
    push_row = scale_in[0] * experts * share
    push = upright(push_row)
    prob = prob_v[...]
    spread = prob * (push - jnp.sum(prob * push, axis=0, keepdims=True))
    named = named_v[...]
    logits = logit_v[...]
    high = jnp.max(jnp.where(named > 0.5, logits, -jnp.inf), axis=0, keepdims=True)
    mix = jnp.where(named > 0.5, jnp.exp(jnp.minimum(logits - high, 0.0)), 0.0)
    mix = mix / jnp.sum(mix, axis=0, keepdims=True)

    def rep_arrival(s_):
        src = lax.rem(me + ep - s_, ep)
        remote(rst.at[src], rbuf.at[src], s_rep.at[src], r_rep.at[src], ep_id(src)).wait_recv()

    loop_ep(rep_arrival)
    dots = jnp.concatenate([rbuf[j, 0:exp_dev, :] for j in range(ep)], axis=0)
    sel = mix * (dots - jnp.sum(mix * dots, axis=0, keepdims=True))
    grad = (spread + sel).astype(BF16)
    lg_out[...] = grad
    lgd[md] = grad

    def lg_copy(s):
        return remote(lgd.at[md], lgd.at[md], s_lg.at[s], r_lg.at[md], (me, dp_peer(s)))

    def lg_arrival(s):
        src = lax.rem(md + dp - s, dp)
        return remote(lgd.at[src], lgd.at[src], s_lg.at[s], r_lg.at[src], (me, src))

    for s in range(1, dp):
        lg_copy(s).start()
    for s in range(1, dp):
        tk_arrival(s).wait_recv()
    for s in range(1, dp):
        lg_arrival(s).wait_recv()
    term = dot_nn(lgd[0], tkr[0])
    for d in range(1, dp):
        term = term + dot_nn(lgd[d], tkr[d])
    for j in range(ep):
        ws[j] = term[j * exp_dev:(j + 1) * exp_dev, :]
    wr[me] = ws[me]
    loop_ep(lambda s_: remote(ws.at[ep_peer(s_)], wr.at[me], s_w.at[s_], r_w.at[me], ep_id(ep_peer(s_))).start())

    def w_arrival(s_):
        src = lax.rem(me + ep - s_, ep)
        remote(ws.at[src], wr.at[src], s_w.at[s_], r_w.at[src], ep_id(src)).wait_recv()

    loop_ep(w_arrival)
    out = lax.fori_loop(1, ep, lambda j, acc: acc + wr[j], wr[0])
    wg_out[...] = out / math.sqrt(token_total)

    loop_ep(lambda s_: idx_copy(s_).wait_send())
    loop_ep(lambda s_: remote(st_ep.at[me], st_ep.at[me], s_se.at[s_], r_se.at[me], ep_id(ep_peer(s_))).wait_send())
    loop_ep(lambda s_: reply(ep_peer(s_)).wait_send())
    loop_ep(lambda s_: remote(ws.at[ep_peer(s_)], wr.at[me], s_w.at[s_], r_w.at[me], ep_id(ep_peer(s_))).wait_send())
    for s in range(1, dp):
        sd_copy(s).wait_send()
        tk_copy(s).wait_send()
        lg_copy(s).wait_send()

    def drain(q, carry):
        for c in range(chunks):
            leaf(q, c).wait_send()

            @pl.when(jnp.logical_and(q <= pos, pos < line - 1))
            def _():
                to_right(q, c).wait_send()

            @pl.when(jnp.logical_and(q >= pos, pos > 0))
            def _():
                to_left(q, c).wait_send()
        return carry

    lax.fori_loop(0, line, drain, 0)


def on_device(tokens, out_grad, indices, expert_rows, router_weight, router_bias, balance_scale):
    tok_dev, width = tokens.shape
    chosen = indices.shape[1]
    experts = router_weight.shape[1]
    exp_dev, cap = expert_rows.shape[1], expert_rows.shape[3]
    ep = lax.axis_size("ep")
    dp = lax.axis_size("dp")
    line = ep // 2
    packed = -(-min(tok_dev, (exp_dev - 1) * cap) // 16) * 16
    widths = tuple(min(CHUNK, width - s) for s in range(0, width, CHUNK))
    chunks = len(widths)
    cfg = (ep, dp, tok_dev, chosen, experts, exp_dev, cap, packed, widths, tok_dev * ep * dp)
    part = width // dp
    rows_t = jnp.transpose(expert_rows[0], (0, 2, 1, 3)).reshape(exp_dev, cap * ep, width)
    vmem = pl.BlockSpec(memory_space=pltpu.VMEM)
    hbm = pl.BlockSpec(memory_space=pl.ANY)
    smem = pl.BlockSpec(memory_space=pltpu.SMEM)
    dma = pltpu.SemaphoreType.DMA
    scratch = [pltpu.VMEM((line, tok_dev, w), BF16) for w in widths]
    scratch += [pltpu.VMEM((line, packed, w), BF16) for w in widths]
    scratch += [pltpu.VMEM((line, packed, w), BF16) for w in widths]
    scratch += [pltpu.VMEM((ep, -(-exp_dev * cap // 16) * 16, w), BF16) for w in widths]
    scratch += [
        pltpu.VMEM((exp_dev, cap * ep, width), BF16),
        pltpu.VMEM((exp_dev, ep * (-(-cap // 8) * 8), widths[0]), F32),
        pltpu.VMEM((ep, chosen, tok_dev), jnp.int32),
        pltpu.VMEM((line, packed, tok_dev), BF16),
        pltpu.VMEM((line, packed, tok_dev), BF16),
        pltpu.VMEM((line, 8, tok_dev), F32),
        pltpu.VMEM((line, 8, packed), F32),
        pltpu.VMEM((line, 8, tok_dev), F32),
        pltpu.VMEM((line, 8, packed), F32),
        pltpu.VMEM((ep, 8, tok_dev), F32),
        pltpu.VMEM((ep, 8, tok_dev), F32),
        pltpu.VMEM((dp, tok_dev, part), BF16),
        pltpu.VMEM((dp, tok_dev, part), BF16),
        pltpu.VMEM((experts, tok_dev), F32),
        pltpu.VMEM((experts, tok_dev), F32),
        pltpu.VMEM((experts, tok_dev), F32),
        pltpu.VMEM((dp, 8, experts), F32),
        pltpu.VMEM((ep, 8, experts), F32),
        pltpu.VMEM((dp, experts, tok_dev), BF16),
        pltpu.VMEM((ep, exp_dev, part), F32),
        pltpu.VMEM((ep, exp_dev, part), F32),
        dma, dma((chunks,)), dma((ep,)), dma((ep,)),
        dma((line, chunks)), dma((line, chunks)), dma((line, chunks)),
        dma((line, chunks)), dma((line, chunks)), dma((ep,)), dma((ep,)),
        dma((dp,)), dma((dp,)), dma((dp,)), dma((dp,)), dma((ep,)), dma((ep,)),
        dma((dp,)), dma((dp,)), dma((ep,)), dma((ep,)),
    ]
    lg, wg, loss = pl.pallas_call(
        functools.partial(kernel, cfg),
        name="router_backward",
        out_shape=(
            jax.ShapeDtypeStruct((experts, tok_dev), BF16),
            jax.ShapeDtypeStruct((exp_dev, part), F32),
            jax.ShapeDtypeStruct((1, 1), F32),
        ),
        in_specs=[vmem, hbm, hbm, vmem, vmem, vmem, smem],
        out_specs=(vmem, vmem, vmem),
        scratch_shapes=scratch,
        compiler_params=pltpu.CompilerParams(
            collective_id=0, has_side_effects=True, vmem_limit_bytes=56 * 1024 * 1024
        ),
    )(indices.T, out_grad, rows_t, tokens, router_weight.T, router_bias.reshape(1, experts), balance_scale)
    token_grad = lax.dot_general(
        lg, router_weight, (((0,), (1,)), ((), ())), preferred_element_type=F32
    ).astype(BF16)
    return (token_grad, wg.T, loss.reshape(1))


def solution(mesh):
    placed = (
        P(("ep", "dp"), None),
        P(("ep", "dp"), None),
        P(("ep", "dp"), None),
        P("dp", "ep", None, None, None),
        P(),
        P(),
        P(),
    )
    return jax.shard_map(
        on_device,
        mesh=mesh,
        in_specs=placed,
        out_specs=(P(("ep", "dp"), None), P("dp", "ep"), P()),
        check_vma=False,
    )
```

```python
import functools
import math

import jax
import jax.numpy as jnp
from jax import lax
from jax.experimental import pallas as pl
from jax.experimental.pallas import tpu as pltpu
from jax.sharding import PartitionSpec as P

MESH = pl.DeviceIdType.MESH
F32 = jnp.float32
BF16 = jnp.bfloat16
CHUNK = 768


def dot_nt(x, y, precision=None):
    return lax.dot_general(
        x, y, (((1,), (1,)), ((), ())), preferred_element_type=F32, precision=precision
    )


def dot_nn(x, y, precision=None):
    return lax.dot_general(
        x, y, (((1,), (0,)), ((), ())), preferred_element_type=F32, precision=precision
    )


def kernel(cfg, *refs):
    ep, dp, tok_dev, chosen, experts, exp_dev, cap, packed, widths, token_total = cfg
    line = ep // 2
    chunks = len(widths)
    starts = [sum(widths[:c]) for c in range(chunks)]
    (idx_in, grad_in, rows_in, tok_in, wt_in, bias_in, scale_in, lg_out, wg_out, loss_out) = refs[:10]
    refs = refs[10:]
    xb = refs[:chunks]
    lsend = refs[chunks:2 * chunks]
    lrecv = refs[2 * chunks:3 * chunks]
    rows_v = refs[3 * chunks:4 * chunks]
    back = refs[4 * chunks:5 * chunks]
    (rows_raw, piled, tgt_r, acc_r, s_back, r_back, idx_all, pin, pout, tgt_x, tgt_p, acc_x, acc_p, rst, rbuf, tks, tkr, logit_v, prob_v,
     named_v, st_dp, st_ep, lgd, ws, wr,
     s_rows, s_own, s_idx, r_idx, s_right, s_left, r_x, s_leaf, r_leaf, s_rep, r_rep,
     s_tk, r_tk, s_sd, r_sd, s_se, r_se, s_lg, r_lg, s_w, r_w) = refs[5 * chunks:]
    me = lax.axis_index("ep")
    md = lax.axis_index("dp")
    pos = me // 2
    side = lax.rem(me, 2)
    mate = pos * 2 + 1 - side
    swapped = range(chunks - 1) if line >= 4 else range(0)
    last = line - 1
    at_end = jnp.logical_or(pos == 0, pos == last)
    near_end = jnp.logical_or(pos == 1, pos == last - 1)
    end = jnp.where(pos * 2 < line, 0, last)
    near = jnp.where(pos * 2 < line, 1, last - 1)

    def ep_id(other):
        return (other, md)

    def remote(src, dst, s, r, dev):
        return pltpu.make_async_remote_copy(
            src_ref=src, dst_ref=dst, send_sem=s, recv_sem=r, device_id=dev, device_id_type=MESH
        )

    def ep_peer(s):
        return lax.rem(me + s, ep)

    def dp_peer(s):
        return lax.rem(md + s, dp)

    own = [
        pltpu.make_async_copy(grad_in.at[:, pl.ds(starts[c], widths[c])], xb[c].at[pos], s_own.at[c])
        for c in range(chunks)
    ]
    for copy in own:
        copy.start()
    rows_copy = pltpu.make_async_copy(rows_in, rows_raw, s_rows)
    rows_copy.start()

    barrier = pltpu.get_barrier_semaphore()

    def greet(s, carry):
        pl.semaphore_signal(barrier, inc=1, device_id=ep_id(ep_peer(s)), device_id_type=MESH)
        return carry

    lax.fori_loop(1, ep, greet, 0)
    for s in range(1, dp):
        pl.semaphore_signal(barrier, inc=1, device_id=(me, dp_peer(s)), device_id_type=MESH)
    pl.semaphore_wait(barrier, ep - 1 + dp - 1)

    def idx_copy(s):
        return remote(idx_in, idx_all.at[me], s_idx.at[s], r_idx.at[me], ep_id(ep_peer(s)))

    def idx_arrival(s):
        src = lax.rem(me + ep - s, ep)
        return remote(idx_in, idx_all.at[src], s_idx.at[s], r_idx.at[src], ep_id(src))

    def loop_ep(fn):
        def body(s, carry):
            fn(s)
            return carry
        lax.fori_loop(1, ep, body, 0)

    def to_right(q, c):
        return remote(xb[c].at[q], xb[c].at[q], s_right.at[q, c], r_x.at[q, c], ep_id(me + 2))

    def to_left(q, c):
        return remote(xb[c].at[q], xb[c].at[q], s_left.at[q, c], r_x.at[q, c], ep_id(me - 2))

    def leaf(q, c):
        return remote(lsend[c].at[q], lrecv[c].at[q], s_leaf.at[q, c], r_leaf.at[q, c], ep_id(mate))

    def send_back(b, c):
        return remote(rows_v[c].at[near * 2 + b], back[c].at[side], s_back.at[b, c], r_back.at[side, c], ep_id(near * 2 + b))

    def from_left(s, c):
        ok = pos - s >= 0
        return jnp.logical_and(ok, pos < last) if s == 1 and c in swapped else ok

    def from_right(s, c):
        ok = pos + s < line
        return jnp.logical_and(ok, pos > 0) if s == 1 and c in swapped else ok

    def reply(j):
        return remote(rst.at[j], rbuf.at[me], s_rep.at[j], r_rep.at[me], ep_id(j))

    loop_ep(lambda s: idx_copy(s).start())
    for c in range(chunks):
        own[c].wait()

        @pl.when(pos < last - (c in swapped))
        def _():
            to_right(pos, c).start()

        @pl.when(pos > 0 + (c in swapped))
        def _():
            to_left(pos, c).start()

    part = tok_in.shape[1] // dp
    for d in range(dp):
        tks[d] = tok_in[:, d * part:(d + 1) * part]

    idx = idx_in[...]
    expert_row = lax.broadcasted_iota(jnp.int32, (experts, tok_dev), 0)
    named = jnp.zeros((experts, tok_dev), F32)
    for k in range(chosen):
        named = named + jnp.where(idx[k:k + 1, :] == expert_row, 1.0, 0.0)
    eye_r = lax.broadcasted_iota(jnp.int32, (experts, experts), 0)
    eye_c = lax.broadcasted_iota(jnp.int32, (experts, experts), 1)

    def upright(line_of):
        return jnp.sum(jnp.where(eye_r == eye_c, line_of, 0.0), axis=1, keepdims=True)

    logits = dot_nt(wt_in[...], tok_in[...]) + upright(bias_in[...])
    top = jnp.max(logits, axis=0, keepdims=True)
    power = jnp.exp(logits - top)
    prob = power / jnp.sum(power, axis=0, keepdims=True)
    logit_v[...] = logits
    prob_v[...] = prob
    named_v[...] = named
    ones = jnp.ones((8, tok_dev), F32)
    count_row = dot_nt(ones, named, lax.Precision.HIGHEST)
    prob_row = dot_nt(ones, prob, lax.Precision.HIGHEST)
    stat_row = lax.broadcasted_iota(jnp.int32, (8, experts), 0)
    st_dp[md] = jnp.where(stat_row == 0, count_row, prob_row)

    def tk_copy(s):
        return remote(tks.at[dp_peer(s)], tkr.at[md], s_tk.at[s], r_tk.at[md], (me, dp_peer(s)))

    def tk_arrival(s):
        src = lax.rem(md + dp - s, dp)
        return remote(tks.at[src], tkr.at[src], s_tk.at[s], r_tk.at[src], (me, src))

    def sd_copy(s):
        return remote(st_dp.at[md], st_dp.at[md], s_sd.at[s], r_sd.at[md], (me, dp_peer(s)))

    def sd_arrival(s):
        src = lax.rem(md + dp - s, dp)
        return remote(st_dp.at[src], st_dp.at[src], s_sd.at[s], r_sd.at[src], (me, src))

    for s in range(1, dp):
        sd_copy(s).start()
    for s in range(1, dp):
        tk_copy(s).start()
    tkr[md] = tks[md]

    t_from = lax.broadcasted_iota(jnp.int32, (tok_dev, tok_dev), 0)
    t_to = lax.broadcasted_iota(jnp.int32, (tok_dev, tok_dev), 1)
    upper = jnp.where(t_from < t_to, 1.0, 0.0).astype(BF16)
    row8 = lax.broadcasted_iota(jnp.int32, (8, tok_dev), 0)
    slot_p = lax.broadcasted_iota(jnp.int32, (packed, tok_dev), 0).astype(F32)

    def plan(table, group):
        who = jnp.where(row8 < exp_dev, group * exp_dev + row8, -2)
        hit = jnp.zeros((8, tok_dev), F32)
        for k in range(chosen):
            hit = hit + jnp.where(table[k:k + 1, :] == who, 1.0, 0.0)
        need = jnp.max(hit, axis=0, keepdims=True)
        stack = jnp.where(row8 == exp_dev, need, hit)
        before = dot_nn(stack.astype(BF16), upper)
        place = jnp.where(need > 0.5, before[exp_dev:exp_dev + 1, :], -1.0)
        target = jnp.where(hit > 0.5, before, -1.0)
        pack = jnp.where(slot_p == place, 1.0, 0.0).astype(BF16)
        return target, pack

    idx_all[me] = idx
    loop_ep(lambda s: idx_arrival(s).wait_recv())

    def plans(q, carry):
        table = idx_all[q * 2 + side]
        target, _ = plan(table, me)
        tgt_x[q] = target
        _, pack = plan(table, mate)
        pout[q] = pack
        target, pack = plan(idx_all[q * 2 + 1 - side], me)
        pin[q] = pack
        tgt_p[q] = dot_nt((target + 1.0).astype(BF16), pack) - 1.0
        acc_x[q] = jnp.zeros((8, tok_dev), F32)
        acc_p[q] = jnp.zeros((8, packed), F32)
        return carry

    lax.fori_loop(0, line, plans, 0)
    for b in range(2):
        tgt_r[b], _ = plan(idx, end * 2 + b)
        acc_r[b] = jnp.zeros((8, tok_dev), F32)
    rows_copy.wait()

    deep = piled.shape[1] // ep
    slot_r = lax.broadcasted_iota(jnp.int32, (deep, cap * ep), 0)
    lies = lax.broadcasted_iota(jnp.int32, (deep, cap * ep), 1)
    order = jnp.concatenate(
        [jnp.where(jnp.logical_and(lies == slot_r * ep + j, slot_r < cap), 1.0, 0.0) for j in range(ep)], axis=0
    ).astype(BF16)
    spare = rows_v[0].shape[1] - exp_dev * cap

    def sort_rows(c):
        w = widths[c]
        for e in range(exp_dev):
            piled[e, :, 0:w] = dot_nn(order, rows_raw[e, :, starts[c]:starts[c] + w])

        def put(j, carry):
            at = pl.ds(pl.multiple_of(j * deep, 8), deep)
            pieces = [piled[e, at, 0:w][0:cap, :] for e in range(exp_dev)]
            if spare:
                pieces.append(jnp.zeros((spare, w), F32))
            rows_v[c][j] = jnp.concatenate(pieces, axis=0).astype(BF16)
            return carry

        lax.fori_loop(0, ep, put, 0)

    def gathered(table, block, target, count):
        height = table.shape[0]
        slot = lax.broadcasted_iota(jnp.int32, (height, count), 0).astype(F32)
        row = lax.broadcasted_iota(jnp.int32, (8, count), 0)
        dots = dot_nt(table, block)
        out = jnp.zeros((8, count), F32)
        for e in range(exp_dev):
            want = jnp.where(target[e:e + 1, :] >= 0.0, target[e:e + 1, :] + e * cap, -1.0)
            one = jnp.sum(jnp.where(slot == want, dots, 0.0), axis=0, keepdims=True)
            out = jnp.where(row == e, one, out)
        return out

    def give_leaf(q, c):
        lsend[c][q] = dot_nn(pout[q], xb[c][q]).astype(BF16)
        leaf(q, c).start()

    def use_block(q, c):
        acc_x[q] += gathered(rows_v[c][q * 2 + side], xb[c][q], tgt_x[q], tok_dev)

    def use_leaf(q, c):
        leaf(q, c).wait_recv()
        acc_p[q] += gathered(rows_v[c][q * 2 + 1 - side], lrecv[c][q], tgt_p[q], packed)

    def answer(j, value):
        rst[j] = value
        reply(j).start()

    def done_block(q):
        answer(q * 2 + side, acc_x[q])

    def done_leaf(q):
        answer(q * 2 + 1 - side, dot_nn(acc_p[q], pin[q].astype(F32), lax.Precision.HIGHEST))

    def leaf_step(s, c):
        def go(q):
            use_leaf(q, c)
            if c == chunks - 1:
                done_leaf(q)
        if s == 0:
            go(pos)
            return

        @pl.when(from_left(s, c))
        def _():
            go(pos - s)

        @pl.when(from_right(s, c))
        def _():
            go(pos + s)

    lag = 2
    steps = [(s, c) for s in range(line) for c in range(chunks)]
    for n, (s, c) in enumerate(steps):
        if s == 0:
            give_leaf(pos, c)
            sort_rows(c)
            if c in swapped:
                @pl.when(at_end)
                def _():
                    for b in range(2):
                        send_back(b, c).start()
            use_block(pos, c)
            if c == chunks - 1:
                rbuf[me] = acc_x[pos]
        else:
            @pl.when(from_left(s, c))
            def _():
                q = pos - s
                to_right(q, c).wait_recv()

                @pl.when(pos < line - 1)
                def _():
                    to_right(q, c).start()

            @pl.when(from_right(s, c))
            def _():
                q = pos + s
                to_left(q, c).wait_recv()

                @pl.when(pos > 0)
                def _():
                    to_left(q, c).start()

            for q, ok in ((pos - s, from_left(s, c)), (pos + s, from_right(s, c))):
                @pl.when(ok)
                def _(q=q):
                    give_leaf(q, c)

            for q, ok in ((pos - s, from_left(s, c)), (pos + s, from_right(s, c))):
                @pl.when(ok)
                def _(q=q):
                    use_block(q, c)
                    if c == chunks - 1:
                        done_block(q)
        if n >= lag:
            leaf_step(*steps[n - lag])
        if s == last and c in swapped:
            @pl.when(near_end)
            def _():
                for b in range(2):
                    remote(back[c].at[b], back[c].at[b], s_back.at[b, c], r_back.at[b, c], ep_id(end * 2 + b)).wait_recv()
                    acc_r[b] += gathered(back[c][b], xb[c][pos], tgt_r[b], tok_dev)
        if n == 1:
            for s_ in range(1, dp):
                sd_arrival(s_).wait_recv()
            total = st_dp[0]
            for d in range(1, dp):
                total = total + st_dp[d]
            st_ep[me] = total
            loop_ep(lambda s_: remote(st_ep.at[me], st_ep.at[me], s_se.at[s_], r_se.at[me], ep_id(ep_peer(s_))).start())
    for n in range(len(steps) - lag, len(steps)):
        leaf_step(*steps[n])

    def se_arrival(s_):
        src = lax.rem(me + ep - s_, ep)
        remote(st_ep.at[src], st_ep.at[src], s_se.at[s_], r_se.at[src], ep_id(src)).wait_recv()

    loop_ep(se_arrival)
    stats = lax.fori_loop(1, ep, lambda j, acc: acc + st_ep[j], st_ep[0])
    share = stats[0:1, :] / (token_total * chosen)
    mean = stats[1:2, :] / token_total
    loss_out[...] = experts * jnp.sum(share * mean, axis=1, keepdims=True)
    push_row = scale_in[0] * experts * share
    push = upright(push_row)
    prob = prob_v[...]
    spread = prob * (push - jnp.sum(prob * push, axis=0, keepdims=True))
    named = named_v[...]
    logits = logit_v[...]
    high = jnp.max(jnp.where(named > 0.5, logits, -jnp.inf), axis=0, keepdims=True)
    mix = jnp.where(named > 0.5, jnp.exp(jnp.minimum(logits - high, 0.0)), 0.0)
    mix = mix / jnp.sum(mix, axis=0, keepdims=True)

    def rep_arrival(s_):
        src = lax.rem(me + ep - s_, ep)
        remote(rst.at[src], rbuf.at[src], s_rep.at[src], r_rep.at[src], ep_id(src)).wait_recv()

    loop_ep(rep_arrival)
    if len(swapped):
        @pl.when(near_end)
        def _():
            for b in range(2):
                rbuf[end * 2 + b] += acc_r[b]
    dots = jnp.concatenate([rbuf[j, 0:exp_dev, :] for j in range(ep)], axis=0)
    sel = mix * (dots - jnp.sum(mix * dots, axis=0, keepdims=True))
    grad = (spread + sel).astype(BF16)
    lg_out[...] = grad
    lgd[md] = grad

    def lg_copy(s):
        return remote(lgd.at[md], lgd.at[md], s_lg.at[s], r_lg.at[md], (me, dp_peer(s)))

    def lg_arrival(s):
        src = lax.rem(md + dp - s, dp)
        return remote(lgd.at[src], lgd.at[src], s_lg.at[s], r_lg.at[src], (me, src))

    for s in range(1, dp):
        lg_copy(s).start()
    for s in range(1, dp):
        tk_arrival(s).wait_recv()
    for s in range(1, dp):
        lg_arrival(s).wait_recv()
    term = dot_nn(lgd[0], tkr[0])
    for d in range(1, dp):
        term = term + dot_nn(lgd[d], tkr[d])
    for j in range(ep):
        ws[j] = term[j * exp_dev:(j + 1) * exp_dev, :]
    wr[me] = ws[me]
    loop_ep(lambda s_: remote(ws.at[ep_peer(s_)], wr.at[me], s_w.at[s_], r_w.at[me], ep_id(ep_peer(s_))).start())

    def w_arrival(s_):
        src = lax.rem(me + ep - s_, ep)
        remote(ws.at[src], wr.at[src], s_w.at[s_], r_w.at[src], ep_id(src)).wait_recv()

    loop_ep(w_arrival)
    out = lax.fori_loop(1, ep, lambda j, acc: acc + wr[j], wr[0])
    wg_out[...] = out / math.sqrt(token_total)

    loop_ep(lambda s_: idx_copy(s_).wait_send())
    loop_ep(lambda s_: remote(st_ep.at[me], st_ep.at[me], s_se.at[s_], r_se.at[me], ep_id(ep_peer(s_))).wait_send())
    loop_ep(lambda s_: reply(ep_peer(s_)).wait_send())
    loop_ep(lambda s_: remote(ws.at[ep_peer(s_)], wr.at[me], s_w.at[s_], r_w.at[me], ep_id(ep_peer(s_))).wait_send())
    for s in range(1, dp):
        sd_copy(s).wait_send()
        tk_copy(s).wait_send()
        lg_copy(s).wait_send()

    def drain(q, carry):
        for c in range(chunks):
            right = jnp.logical_and(q <= pos, pos < last)
            left = jnp.logical_and(q >= pos, pos > 0)
            used = q >= 0
            if c in swapped:
                right = jnp.logical_and(right, jnp.logical_or(q < pos, pos < last - 1))
                left = jnp.logical_and(left, jnp.logical_or(q > pos, pos > 1))
                used = jnp.logical_not(jnp.logical_and(at_end, q == near))

            @pl.when(used)
            def _():
                leaf(q, c).wait_send()

            @pl.when(right)
            def _():
                to_right(q, c).wait_send()

            @pl.when(left)
            def _():
                to_left(q, c).wait_send()
        return carry

    if len(swapped):
        @pl.when(at_end)
        def _():
            for c in swapped:
                for b in range(2):
                    send_back(b, c).wait_send()
    lax.fori_loop(0, line, drain, 0)


def on_device(tokens, out_grad, indices, expert_rows, router_weight, router_bias, balance_scale):
    tok_dev, width = tokens.shape
    chosen = indices.shape[1]
    experts = router_weight.shape[1]
    exp_dev, cap = expert_rows.shape[1], expert_rows.shape[3]
    ep = lax.axis_size("ep")
    dp = lax.axis_size("dp")
    line = ep // 2
    packed = -(-min(tok_dev, (exp_dev - 1) * cap) // 16) * 16
    widths = tuple(min(CHUNK, width - s) for s in range(0, width, CHUNK))
    chunks = len(widths)
    cfg = (ep, dp, tok_dev, chosen, experts, exp_dev, cap, packed, widths, tok_dev * ep * dp)
    part = width // dp
    rows_t = jnp.transpose(expert_rows[0], (0, 2, 1, 3)).reshape(exp_dev, cap * ep, width)
    vmem = pl.BlockSpec(memory_space=pltpu.VMEM)
    hbm = pl.BlockSpec(memory_space=pl.ANY)
    smem = pl.BlockSpec(memory_space=pltpu.SMEM)
    dma = pltpu.SemaphoreType.DMA
    scratch = [pltpu.VMEM((line, tok_dev, w), BF16) for w in widths]
    scratch += [pltpu.VMEM((line, packed, w), BF16) for w in widths]
    scratch += [pltpu.VMEM((line, packed, w), BF16) for w in widths]
    scratch += [pltpu.VMEM((ep, -(-exp_dev * cap // 16) * 16, w), BF16) for w in widths]
    scratch += [pltpu.VMEM((2, -(-exp_dev * cap // 16) * 16, w), BF16) for w in widths]
    scratch += [
        pltpu.VMEM((exp_dev, cap * ep, width), BF16),
        pltpu.VMEM((exp_dev, ep * (-(-cap // 8) * 8), widths[0]), F32),
        pltpu.VMEM((2, 8, tok_dev), F32),
        pltpu.VMEM((2, 8, tok_dev), F32),
        dma((2, chunks)), dma((2, chunks)),
        pltpu.VMEM((ep, chosen, tok_dev), jnp.int32),
        pltpu.VMEM((line, packed, tok_dev), BF16),
        pltpu.VMEM((line, packed, tok_dev), BF16),
        pltpu.VMEM((line, 8, tok_dev), F32),
        pltpu.VMEM((line, 8, packed), F32),
        pltpu.VMEM((line, 8, tok_dev), F32),
        pltpu.VMEM((line, 8, packed), F32),
        pltpu.VMEM((ep, 8, tok_dev), F32),
        pltpu.VMEM((ep, 8, tok_dev), F32),
        pltpu.VMEM((dp, tok_dev, part), BF16),
        pltpu.VMEM((dp, tok_dev, part), BF16),
        pltpu.VMEM((experts, tok_dev), F32),
        pltpu.VMEM((experts, tok_dev), F32),
        pltpu.VMEM((experts, tok_dev), F32),
        pltpu.VMEM((dp, 8, experts), F32),
        pltpu.VMEM((ep, 8, experts), F32),
        pltpu.VMEM((dp, experts, tok_dev), BF16),
        pltpu.VMEM((ep, exp_dev, part), F32),
        pltpu.VMEM((ep, exp_dev, part), F32),
        dma, dma((chunks,)), dma((ep,)), dma((ep,)),
        dma((line, chunks)), dma((line, chunks)), dma((line, chunks)),
        dma((line, chunks)), dma((line, chunks)), dma((ep,)), dma((ep,)),
        dma((dp,)), dma((dp,)), dma((dp,)), dma((dp,)), dma((ep,)), dma((ep,)),
        dma((dp,)), dma((dp,)), dma((ep,)), dma((ep,)),
    ]
    lg, wg, loss = pl.pallas_call(
        functools.partial(kernel, cfg),
        name="router_backward",
        out_shape=(
            jax.ShapeDtypeStruct((experts, tok_dev), BF16),
            jax.ShapeDtypeStruct((exp_dev, part), F32),
            jax.ShapeDtypeStruct((1, 1), F32),
        ),
        in_specs=[vmem, hbm, hbm, vmem, vmem, vmem, smem],
        out_specs=(vmem, vmem, vmem),
        scratch_shapes=scratch,
        compiler_params=pltpu.CompilerParams(
            collective_id=0, has_side_effects=True, vmem_limit_bytes=56 * 1024 * 1024
        ),
    )(indices.T, out_grad, rows_t, tokens, router_weight.T, router_bias.reshape(1, experts), balance_scale)
    token_grad = lax.dot_general(
        lg, router_weight, (((0,), (1,)), ((), ())), preferred_element_type=F32
    ).astype(BF16)
    return (token_grad, wg.T, loss.reshape(1))


def solution(mesh):
    placed = (
        P(("ep", "dp"), None),
        P(("ep", "dp"), None),
        P(("ep", "dp"), None),
        P("dp", "ep", None, None, None),
        P(),
        P(),
        P(),
    )
    return jax.shard_map(
        on_device,
        mesh=mesh,
        in_specs=placed,
        out_specs=(P(("ep", "dp"), None), P("dp", "ep"), P()),
        check_vma=False,
    )
```

```python
import functools
import math

import jax
import jax.numpy as jnp
from jax import lax
from jax.experimental import pallas as pl
from jax.experimental.pallas import tpu as pltpu
from jax.sharding import PartitionSpec as P

MESH = pl.DeviceIdType.MESH
F32 = jnp.float32
BF16 = jnp.bfloat16
CHUNK = 768


def dot_nt(x, y, precision=None):
    return lax.dot_general(
        x, y, (((1,), (1,)), ((), ())), preferred_element_type=F32, precision=precision
    )


def dot_nn(x, y, precision=None):
    return lax.dot_general(
        x, y, (((1,), (0,)), ((), ())), preferred_element_type=F32, precision=precision
    )


def kernel(cfg, *refs):
    ep, dp, tok_dev, chosen, experts, exp_dev, cap, packed, widths, token_total = cfg
    line = ep // 2
    chunks = len(widths)
    starts = [sum(widths[:c]) for c in range(chunks)]
    (idx_in, grad_in, rows_in, tok_in, wt_in, bias_in, scale_in, lg_out, wg_out, loss_out) = refs[:10]
    refs = refs[10:]
    xb = refs[:chunks]
    lsend = refs[chunks:2 * chunks]
    lrecv = refs[2 * chunks:3 * chunks]
    rows_v = refs[3 * chunks:4 * chunks]
    back = refs[4 * chunks:5 * chunks]
    (rows_raw, piled, tgt_r, acc_r, s_back, r_back, idx_all, pin, pout, tgt_x, tgt_p, acc_x, acc_p, rst, rbuf, tks, tkr, logit_v, prob_v,
     named_v, st_dp, st_ep, lgd, ws, wr,
     s_rows, s_own, s_idx, r_idx, s_right, s_left, r_x, s_leaf, r_leaf, s_rep, r_rep,
     s_tk, r_tk, s_sd, r_sd, s_se, r_se, s_lg, r_lg, s_w, r_w) = refs[5 * chunks:]
    me = lax.axis_index("ep")
    md = lax.axis_index("dp")
    pos = me // 2
    side = lax.rem(me, 2)
    mate = pos * 2 + 1 - side
    swapped = range(min(1, chunks - 1)) if line >= 4 else range(0)
    last = line - 1
    at_end = jnp.logical_or(pos == 0, pos == last)
    near_end = jnp.logical_or(pos == 1, pos == last - 1)
    end = jnp.where(pos * 2 < line, 0, last)
    near = jnp.where(pos * 2 < line, 1, last - 1)

    def ep_id(other):
        return (other, md)

    def remote(src, dst, s, r, dev):
        return pltpu.make_async_remote_copy(
            src_ref=src, dst_ref=dst, send_sem=s, recv_sem=r, device_id=dev, device_id_type=MESH
        )

    def ep_peer(s):
        return lax.rem(me + s, ep)

    def dp_peer(s):
        return lax.rem(md + s, dp)

    own = [
        pltpu.make_async_copy(grad_in.at[:, pl.ds(starts[c], widths[c])], xb[c].at[pos], s_own.at[c])
        for c in range(chunks)
    ]
    for copy in own:
        copy.start()
    rows_copy = pltpu.make_async_copy(rows_in, rows_raw, s_rows)
    rows_copy.start()

    barrier = pltpu.get_barrier_semaphore()

    def greet(s, carry):
        pl.semaphore_signal(barrier, inc=1, device_id=ep_id(ep_peer(s)), device_id_type=MESH)
        return carry

    lax.fori_loop(1, ep, greet, 0)
    for s in range(1, dp):
        pl.semaphore_signal(barrier, inc=1, device_id=(me, dp_peer(s)), device_id_type=MESH)
    pl.semaphore_wait(barrier, ep - 1 + dp - 1)

    def idx_copy(s):
        return remote(idx_in, idx_all.at[me], s_idx.at[s], r_idx.at[me], ep_id(ep_peer(s)))

    def idx_arrival(s):
        src = lax.rem(me + ep - s, ep)
        return remote(idx_in, idx_all.at[src], s_idx.at[s], r_idx.at[src], ep_id(src))

    def loop_ep(fn):
        def body(s, carry):
            fn(s)
            return carry
        lax.fori_loop(1, ep, body, 0)

    def to_right(q, c):
        return remote(xb[c].at[q], xb[c].at[q], s_right.at[q, c], r_x.at[q, c], ep_id(me + 2))

    def to_left(q, c):
        return remote(xb[c].at[q], xb[c].at[q], s_left.at[q, c], r_x.at[q, c], ep_id(me - 2))

    def leaf(q, c):
        return remote(lsend[c].at[q], lrecv[c].at[q], s_leaf.at[q, c], r_leaf.at[q, c], ep_id(mate))

    def send_back(b, c):
        return remote(rows_v[c].at[near * 2 + b], back[c].at[side], s_back.at[b, c], r_back.at[side, c], ep_id(near * 2 + b))

    def from_left(s, c):
        ok = pos - s >= 0
        return jnp.logical_and(ok, pos < last) if s == 1 and c in swapped else ok

    def from_right(s, c):
        ok = pos + s < line
        return jnp.logical_and(ok, pos > 0) if s == 1 and c in swapped else ok

    def reply(j):
        return remote(rst.at[j], rbuf.at[me], s_rep.at[j], r_rep.at[me], ep_id(j))

    loop_ep(lambda s: idx_copy(s).start())
    for c in range(chunks):
        own[c].wait()

        @pl.when(pos < last - (c in swapped))
        def _():
            to_right(pos, c).start()

        @pl.when(pos > 0 + (c in swapped))
        def _():
            to_left(pos, c).start()

    part = tok_in.shape[1] // dp
    for d in range(dp):
        tks[d] = tok_in[:, d * part:(d + 1) * part]

    idx = idx_in[...]
    expert_row = lax.broadcasted_iota(jnp.int32, (experts, tok_dev), 0)
    named = jnp.zeros((experts, tok_dev), F32)
    for k in range(chosen):
        named = named + jnp.where(idx[k:k + 1, :] == expert_row, 1.0, 0.0)
    eye_r = lax.broadcasted_iota(jnp.int32, (experts, experts), 0)
    eye_c = lax.broadcasted_iota(jnp.int32, (experts, experts), 1)

    def upright(line_of):
        return jnp.sum(jnp.where(eye_r == eye_c, line_of, 0.0), axis=1, keepdims=True)

    logits = dot_nt(wt_in[...], tok_in[...]) + upright(bias_in[...])
    top = jnp.max(logits, axis=0, keepdims=True)
    power = jnp.exp(logits - top)
    prob = power / jnp.sum(power, axis=0, keepdims=True)
    logit_v[...] = logits
    prob_v[...] = prob
    named_v[...] = named
    ones = jnp.ones((8, tok_dev), F32)
    count_row = dot_nt(ones, named, lax.Precision.HIGHEST)
    prob_row = dot_nt(ones, prob, lax.Precision.HIGHEST)
    stat_row = lax.broadcasted_iota(jnp.int32, (8, experts), 0)
    st_dp[md] = jnp.where(stat_row == 0, count_row, prob_row)

    def tk_copy(s):
        return remote(tks.at[dp_peer(s)], tkr.at[md], s_tk.at[s], r_tk.at[md], (me, dp_peer(s)))

    def tk_arrival(s):
        src = lax.rem(md + dp - s, dp)
        return remote(tks.at[src], tkr.at[src], s_tk.at[s], r_tk.at[src], (me, src))

    def sd_copy(s):
        return remote(st_dp.at[md], st_dp.at[md], s_sd.at[s], r_sd.at[md], (me, dp_peer(s)))

    def sd_arrival(s):
        src = lax.rem(md + dp - s, dp)
        return remote(st_dp.at[src], st_dp.at[src], s_sd.at[s], r_sd.at[src], (me, src))

    for s in range(1, dp):
        sd_copy(s).start()
    for s in range(1, dp):
        tk_copy(s).start()
    tkr[md] = tks[md]

    t_from = lax.broadcasted_iota(jnp.int32, (tok_dev, tok_dev), 0)
    t_to = lax.broadcasted_iota(jnp.int32, (tok_dev, tok_dev), 1)
    upper = jnp.where(t_from < t_to, 1.0, 0.0).astype(BF16)
    row8 = lax.broadcasted_iota(jnp.int32, (8, tok_dev), 0)
    slot_p = lax.broadcasted_iota(jnp.int32, (packed, tok_dev), 0).astype(F32)

    def plan(table, group):
        who = jnp.where(row8 < exp_dev, group * exp_dev + row8, -2)
        hit = jnp.zeros((8, tok_dev), F32)
        for k in range(chosen):
            hit = hit + jnp.where(table[k:k + 1, :] == who, 1.0, 0.0)
        need = jnp.max(hit, axis=0, keepdims=True)
        stack = jnp.where(row8 == exp_dev, need, hit)
        before = dot_nn(stack.astype(BF16), upper)
        place = jnp.where(need > 0.5, before[exp_dev:exp_dev + 1, :], -1.0)
        target = jnp.where(hit > 0.5, before, -1.0)
        pack = jnp.where(slot_p == place, 1.0, 0.0).astype(BF16)
        return target, pack

    idx_all[me] = idx
    loop_ep(lambda s: idx_arrival(s).wait_recv())

    def plans(q, carry):
        table = idx_all[q * 2 + side]
        target, _ = plan(table, me)
        tgt_x[q] = target
        _, pack = plan(table, mate)
        pout[q] = pack
        target, pack = plan(idx_all[q * 2 + 1 - side], me)
        pin[q] = pack
        tgt_p[q] = dot_nt((target + 1.0).astype(BF16), pack) - 1.0
        acc_x[q] = jnp.zeros((8, tok_dev), F32)
        acc_p[q] = jnp.zeros((8, packed), F32)
        return carry

    lax.fori_loop(0, line, plans, 0)
    for b in range(2):
        tgt_r[b], _ = plan(idx, end * 2 + b)
        acc_r[b] = jnp.zeros((8, tok_dev), F32)
    rows_copy.wait()

    deep = piled.shape[1] // ep
    slot_r = lax.broadcasted_iota(jnp.int32, (deep, cap * ep), 0)
    lies = lax.broadcasted_iota(jnp.int32, (deep, cap * ep), 1)
    order = jnp.concatenate(
        [jnp.where(jnp.logical_and(lies == slot_r * ep + j, slot_r < cap), 1.0, 0.0) for j in range(ep)], axis=0
    ).astype(BF16)
    spare = rows_v[0].shape[1] - exp_dev * cap

    def sort_rows(c):
        w = widths[c]
        for e in range(exp_dev):
            piled[e, :, 0:w] = dot_nn(order, rows_raw[e, :, starts[c]:starts[c] + w])

        def put(j, carry):
            at = pl.ds(pl.multiple_of(j * deep, 8), deep)
            pieces = [piled[e, at, 0:w][0:cap, :] for e in range(exp_dev)]
            if spare:
                pieces.append(jnp.zeros((spare, w), F32))
            rows_v[c][j] = jnp.concatenate(pieces, axis=0).astype(BF16)
            return carry

        lax.fori_loop(0, ep, put, 0)

    def gathered(table, block, target, count):
        height = table.shape[0]
        slot = lax.broadcasted_iota(jnp.int32, (height, count), 0).astype(F32)
        row = lax.broadcasted_iota(jnp.int32, (8, count), 0)
        dots = dot_nt(table, block)
        out = jnp.zeros((8, count), F32)
        for e in range(exp_dev):
            want = jnp.where(target[e:e + 1, :] >= 0.0, target[e:e + 1, :] + e * cap, -1.0)
            one = jnp.sum(jnp.where(slot == want, dots, 0.0), axis=0, keepdims=True)
            out = jnp.where(row == e, one, out)
        return out

    def give_leaf(q, c):
        lsend[c][q] = dot_nn(pout[q], xb[c][q]).astype(BF16)
        leaf(q, c).start()

    def use_block(q, c):
        acc_x[q] += gathered(rows_v[c][q * 2 + side], xb[c][q], tgt_x[q], tok_dev)

    def use_leaf(q, c):
        leaf(q, c).wait_recv()
        acc_p[q] += gathered(rows_v[c][q * 2 + 1 - side], lrecv[c][q], tgt_p[q], packed)

    def answer(j, value):
        rst[j] = value
        reply(j).start()

    def done_block(q):
        answer(q * 2 + side, acc_x[q])

    def done_leaf(q):
        answer(q * 2 + 1 - side, dot_nn(acc_p[q], pin[q].astype(F32), lax.Precision.HIGHEST))

    def leaf_step(s, c):
        def go(q):
            use_leaf(q, c)
            if c == chunks - 1:
                done_leaf(q)
        if s == 0:
            go(pos)
            return

        @pl.when(from_left(s, c))
        def _():
            go(pos - s)

        @pl.when(from_right(s, c))
        def _():
            go(pos + s)

    lag = 2
    steps = [(s, c) for s in range(line) for c in range(chunks)]
    for n, (s, c) in enumerate(steps):
        if s == 0:
            give_leaf(pos, c)
            sort_rows(c)
            if c in swapped:
                @pl.when(at_end)
                def _():
                    for b in range(2):
                        send_back(b, c).start()
            use_block(pos, c)
            if c == chunks - 1:
                rbuf[me] = acc_x[pos]
        else:
            @pl.when(from_left(s, c))
            def _():
                q = pos - s
                to_right(q, c).wait_recv()

                @pl.when(pos < line - 1)
                def _():
                    to_right(q, c).start()

            @pl.when(from_right(s, c))
            def _():
                q = pos + s
                to_left(q, c).wait_recv()

                @pl.when(pos > 0)
                def _():
                    to_left(q, c).start()

            for q, ok in ((pos - s, from_left(s, c)), (pos + s, from_right(s, c))):
                @pl.when(ok)
                def _(q=q):
                    give_leaf(q, c)

            for q, ok in ((pos - s, from_left(s, c)), (pos + s, from_right(s, c))):
                @pl.when(ok)
                def _(q=q):
                    use_block(q, c)
                    if c == chunks - 1:
                        done_block(q)
        if n >= lag:
            leaf_step(*steps[n - lag])
        if s == last and c in swapped:
            @pl.when(near_end)
            def _():
                for b in range(2):
                    remote(back[c].at[b], back[c].at[b], s_back.at[b, c], r_back.at[b, c], ep_id(end * 2 + b)).wait_recv()
                    acc_r[b] += gathered(back[c][b], xb[c][pos], tgt_r[b], tok_dev)
        if n == 1:
            for s_ in range(1, dp):
                sd_arrival(s_).wait_recv()
            total = st_dp[0]
            for d in range(1, dp):
                total = total + st_dp[d]
            st_ep[me] = total
            loop_ep(lambda s_: remote(st_ep.at[me], st_ep.at[me], s_se.at[s_], r_se.at[me], ep_id(ep_peer(s_))).start())
    for n in range(len(steps) - lag, len(steps)):
        leaf_step(*steps[n])

    def se_arrival(s_):
        src = lax.rem(me + ep - s_, ep)
        remote(st_ep.at[src], st_ep.at[src], s_se.at[s_], r_se.at[src], ep_id(src)).wait_recv()

    loop_ep(se_arrival)
    stats = lax.fori_loop(1, ep, lambda j, acc: acc + st_ep[j], st_ep[0])
    share = stats[0:1, :] / (token_total * chosen)
    mean = stats[1:2, :] / token_total
    loss_out[...] = experts * jnp.sum(share * mean, axis=1, keepdims=True)
    push_row = scale_in[0] * experts * share
    push = upright(push_row)
    prob = prob_v[...]
    spread = prob * (push - jnp.sum(prob * push, axis=0, keepdims=True))
    named = named_v[...]
    logits = logit_v[...]
    high = jnp.max(jnp.where(named > 0.5, logits, -jnp.inf), axis=0, keepdims=True)
    mix = jnp.where(named > 0.5, jnp.exp(jnp.minimum(logits - high, 0.0)), 0.0)
    mix = mix / jnp.sum(mix, axis=0, keepdims=True)

    def rep_arrival(s_):
        src = lax.rem(me + ep - s_, ep)
        remote(rst.at[src], rbuf.at[src], s_rep.at[src], r_rep.at[src], ep_id(src)).wait_recv()

    loop_ep(rep_arrival)
    if len(swapped):
        @pl.when(near_end)
        def _():
            for b in range(2):
                rbuf[end * 2 + b] += acc_r[b]
    dots = jnp.concatenate([rbuf[j, 0:exp_dev, :] for j in range(ep)], axis=0)
    sel = mix * (dots - jnp.sum(mix * dots, axis=0, keepdims=True))
    grad = (spread + sel).astype(BF16)
    lg_out[...] = grad
    lgd[md] = grad

    def lg_copy(s):
        return remote(lgd.at[md], lgd.at[md], s_lg.at[s], r_lg.at[md], (me, dp_peer(s)))

    def lg_arrival(s):
        src = lax.rem(md + dp - s, dp)
        return remote(lgd.at[src], lgd.at[src], s_lg.at[s], r_lg.at[src], (me, src))

    for s in range(1, dp):
        lg_copy(s).start()
    for s in range(1, dp):
        tk_arrival(s).wait_recv()
    for s in range(1, dp):
        lg_arrival(s).wait_recv()
    term = dot_nn(lgd[0], tkr[0])
    for d in range(1, dp):
        term = term + dot_nn(lgd[d], tkr[d])
    for j in range(ep):
        ws[j] = term[j * exp_dev:(j + 1) * exp_dev, :]
    wr[me] = ws[me]
    loop_ep(lambda s_: remote(ws.at[ep_peer(s_)], wr.at[me], s_w.at[s_], r_w.at[me], ep_id(ep_peer(s_))).start())

    def w_arrival(s_):
        src = lax.rem(me + ep - s_, ep)
        remote(ws.at[src], wr.at[src], s_w.at[s_], r_w.at[src], ep_id(src)).wait_recv()

    loop_ep(w_arrival)
    out = lax.fori_loop(1, ep, lambda j, acc: acc + wr[j], wr[0])
    wg_out[...] = out / math.sqrt(token_total)

    loop_ep(lambda s_: idx_copy(s_).wait_send())
    loop_ep(lambda s_: remote(st_ep.at[me], st_ep.at[me], s_se.at[s_], r_se.at[me], ep_id(ep_peer(s_))).wait_send())
    loop_ep(lambda s_: reply(ep_peer(s_)).wait_send())
    loop_ep(lambda s_: remote(ws.at[ep_peer(s_)], wr.at[me], s_w.at[s_], r_w.at[me], ep_id(ep_peer(s_))).wait_send())
    for s in range(1, dp):
        sd_copy(s).wait_send()
        tk_copy(s).wait_send()
        lg_copy(s).wait_send()

    def drain(q, carry):
        for c in range(chunks):
            right = jnp.logical_and(q <= pos, pos < last)
            left = jnp.logical_and(q >= pos, pos > 0)
            used = q >= 0
            if c in swapped:
                right = jnp.logical_and(right, jnp.logical_or(q < pos, pos < last - 1))
                left = jnp.logical_and(left, jnp.logical_or(q > pos, pos > 1))
                used = jnp.logical_not(jnp.logical_and(at_end, q == near))

            @pl.when(used)
            def _():
                leaf(q, c).wait_send()

            @pl.when(right)
            def _():
                to_right(q, c).wait_send()

            @pl.when(left)
            def _():
                to_left(q, c).wait_send()
        return carry

    if len(swapped):
        @pl.when(at_end)
        def _():
            for c in swapped:
                for b in range(2):
                    send_back(b, c).wait_send()
    lax.fori_loop(0, line, drain, 0)


def on_device(tokens, out_grad, indices, expert_rows, router_weight, router_bias, balance_scale):
    tok_dev, width = tokens.shape
    chosen = indices.shape[1]
    experts = router_weight.shape[1]
    exp_dev, cap = expert_rows.shape[1], expert_rows.shape[3]
    ep = lax.axis_size("ep")
    dp = lax.axis_size("dp")
    line = ep // 2
    packed = -(-min(tok_dev, (exp_dev - 1) * cap) // 16) * 16
    widths = tuple(min(CHUNK, width - s) for s in range(0, width, CHUNK))
    chunks = len(widths)
    cfg = (ep, dp, tok_dev, chosen, experts, exp_dev, cap, packed, widths, tok_dev * ep * dp)
    part = width // dp
    rows_t = jnp.transpose(expert_rows[0], (0, 2, 1, 3)).reshape(exp_dev, cap * ep, width)
    vmem = pl.BlockSpec(memory_space=pltpu.VMEM)
    hbm = pl.BlockSpec(memory_space=pl.ANY)
    smem = pl.BlockSpec(memory_space=pltpu.SMEM)
    dma = pltpu.SemaphoreType.DMA
    scratch = [pltpu.VMEM((line, tok_dev, w), BF16) for w in widths]
    scratch += [pltpu.VMEM((line, packed, w), BF16) for w in widths]
    scratch += [pltpu.VMEM((line, packed, w), BF16) for w in widths]
    scratch += [pltpu.VMEM((ep, -(-exp_dev * cap // 16) * 16, w), BF16) for w in widths]
    scratch += [pltpu.VMEM((2, -(-exp_dev * cap // 16) * 16, w), BF16) for w in widths]
    scratch += [
        pltpu.VMEM((exp_dev, cap * ep, width), BF16),
        pltpu.VMEM((exp_dev, ep * (-(-cap // 8) * 8), widths[0]), F32),
        pltpu.VMEM((2, 8, tok_dev), F32),
        pltpu.VMEM((2, 8, tok_dev), F32),
        dma((2, chunks)), dma((2, chunks)),
        pltpu.VMEM((ep, chosen, tok_dev), jnp.int32),
        pltpu.VMEM((line, packed, tok_dev), BF16),
        pltpu.VMEM((line, packed, tok_dev), BF16),
        pltpu.VMEM((line, 8, tok_dev), F32),
        pltpu.VMEM((line, 8, packed), F32),
        pltpu.VMEM((line, 8, tok_dev), F32),
        pltpu.VMEM((line, 8, packed), F32),
        pltpu.VMEM((ep, 8, tok_dev), F32),
        pltpu.VMEM((ep, 8, tok_dev), F32),
        pltpu.VMEM((dp, tok_dev, part), BF16),
        pltpu.VMEM((dp, tok_dev, part), BF16),
        pltpu.VMEM((experts, tok_dev), F32),
        pltpu.VMEM((experts, tok_dev), F32),
        pltpu.VMEM((experts, tok_dev), F32),
        pltpu.VMEM((dp, 8, experts), F32),
        pltpu.VMEM((ep, 8, experts), F32),
        pltpu.VMEM((dp, experts, tok_dev), BF16),
        pltpu.VMEM((ep, exp_dev, part), F32),
        pltpu.VMEM((ep, exp_dev, part), F32),
        dma, dma((chunks,)), dma((ep,)), dma((ep,)),
        dma((line, chunks)), dma((line, chunks)), dma((line, chunks)),
        dma((line, chunks)), dma((line, chunks)), dma((ep,)), dma((ep,)),
        dma((dp,)), dma((dp,)), dma((dp,)), dma((dp,)), dma((ep,)), dma((ep,)),
        dma((dp,)), dma((dp,)), dma((ep,)), dma((ep,)),
    ]
    lg, wg, loss = pl.pallas_call(
        functools.partial(kernel, cfg),
        name="router_backward",
        out_shape=(
            jax.ShapeDtypeStruct((experts, tok_dev), BF16),
            jax.ShapeDtypeStruct((exp_dev, part), F32),
            jax.ShapeDtypeStruct((1, 1), F32),
        ),
        in_specs=[vmem, hbm, hbm, vmem, vmem, vmem, smem],
        out_specs=(vmem, vmem, vmem),
        scratch_shapes=scratch,
        compiler_params=pltpu.CompilerParams(
            collective_id=0, has_side_effects=True, vmem_limit_bytes=56 * 1024 * 1024
        ),
    )(indices.T, out_grad, rows_t, tokens, router_weight.T, router_bias.reshape(1, experts), balance_scale)
    token_grad = lax.dot_general(
        lg, router_weight, (((0,), (1,)), ((), ())), preferred_element_type=F32
    ).astype(BF16)
    return (token_grad, wg.T, loss.reshape(1))


def solution(mesh):
    placed = (
        P(("ep", "dp"), None),
        P(("ep", "dp"), None),
        P(("ep", "dp"), None),
        P("dp", "ep", None, None, None),
        P(),
        P(),
        P(),
    )
    return jax.shard_map(
        on_device,
        mesh=mesh,
        in_specs=placed,
        out_specs=(P(("ep", "dp"), None), P("dp", "ep"), P()),
        check_vma=False,
    )
```
